128 devices in a mesh: gx: 8 (over x, core), gy: 4 (over z), gz: 4 (over y).
Axes of the slice: x: 4, y: 4, z: 4, core: 2. Of those that a mesh axis runs over, the one named last changes fastest.
Arguments:
- right_side: float32 [512, 256, 1024], P('gx', 'gy', 'gz'), may hold values from -5 to 7
- initial_guess: float32 [512, 256, 1024], P('gx', 'gy', 'gz'), may hold values from -5 to 7
Outputs:
- solution: float32 [512, 256, 1024], P('gx', 'gy', 'gz')
The draws below stay inside these ranges and needn't reach their ends.
All inputs are finite; a program needn't handle non-finite values.
Results may differ from the reference program's by a relative error of at most 0.000028.
Values sent between devices are 32-bit elements; how exact they have to be, the bound alone decides.
No kernel may reach another device: no remote copies, remote signals or barrier semaphores. Data moves between devices by JAX's collectives and lax.ppermute only.
A program may use at most 128 MiB of HBM per device.

```python
import jax
import jax.numpy as jnp

COARSE_SWEEPS = 6
NX = 512
NY = 256
NZ = 1024


def ramp_field(key, rising):
    noise = jnp.clip(jax.random.normal(key, (NX, NY, NZ), jnp.float32), -5.0, 5.0)
    position = jnp.arange(NX, dtype=jnp.float32) / NX
    if rising:
        offset = 0.5 + position
    else:
        offset = 1.5 - position
    return noise + offset[:, None, None]


def draw_right_side(key, part):
    return ramp_field(jax.random.fold_in(key, 11), True)


def draw_initial_guess(key, part):
    return ramp_field(jax.random.fold_in(key, 23), False)


def setup_inputs(seed: int = 0) -> dict:
    streams_of = jax.random.split(jax.random.key(seed), 3)
    return {
        "right_side": draw_right_side(jax.random.fold_in(streams_of[2], 71), 0),
        "initial_guess": draw_initial_guess(jax.random.fold_in(streams_of[2], 71), 0),
    }


relax_weight = 0.8


def neighbours(values):
    total = jnp.roll(values, -1, 0) + jnp.roll(values, 1, 0)
    total = total + jnp.roll(values, -1, 1) + jnp.roll(values, 1, 1)
    total = total + jnp.roll(values, -1, 2) + jnp.roll(values, 1, 2)
    return total


def relax_step(centre, beside, source, level_scale):
    return centre + relax_weight * (source / (6.0 * level_scale) - centre + beside / 6.0)


def defect_of(centre, beside, source, level_scale):
    return source - level_scale * (6.0 * centre - beside)


def restrict_grid(values):
    for along in range(3):
        count_half = values.shape[along] // 2
        on_points = jax.lax.slice_in_dim(values, 0, 2 * count_half, 2, along)
        between = jax.lax.slice_in_dim(values, 1, 2 * count_half, 2, along)
        lower_side = jnp.roll(between, 1, along)
        values = 0.25 * lower_side + 0.5 * on_points + 0.25 * between
    return values


def prolong_grid(values):
    for along in range(3):
        between = 0.5 * (values + jnp.roll(values, -1, along))
        stacked = jnp.stack([values, between], along + 1)
        new_shape = list(values.shape)
        new_shape[along] = 2 * new_shape[along]
        values = stacked.reshape(new_shape)
    return values


def smoothed(approx, source, level_scale):
    return relax_step(approx, neighbours(approx), source, level_scale)


def multigrid_cycle(approx, source, grid_level):
    level_scale = 0.25 ** grid_level
    if grid_level == 2:
        approx = smoothed(jnp.zeros_like(source), source, level_scale)
        for sweep_index in range(COARSE_SWEEPS - 1):
            approx = smoothed(approx, source, level_scale)
        return approx
    approx = smoothed(smoothed(approx, source, level_scale), source, level_scale)
    defect_field = defect_of(approx, neighbours(approx), source, level_scale)
    coarse_source = restrict_grid(defect_field)
    correction = multigrid_cycle(jnp.zeros_like(coarse_source), coarse_source, grid_level + 1)
    approx = approx + prolong_grid(correction)
    return smoothed(smoothed(approx, source, level_scale), source, level_scale)


def reference(right_side, initial_guess):
    cell_count = NX * NY * NZ
    source = right_side - jnp.sum(right_side) / cell_count
    approx = initial_guess - jnp.sum(initial_guess) / cell_count
    return multigrid_cycle(approx, source, 0)
```

```python
import jax
import jax.numpy as jnp
from jax import lax
from jax.experimental import pallas as pl
from jax.experimental.pallas import tpu as pltpu
from jax.sharding import PartitionSpec as P
import numpy as np

f32 = jnp.float32
KEEP = 0.2
SIDE = 0.8 / 6.0
B0 = 0.8 / 6.0
B1 = 0.8 / (6.0 * 0.25)
B2 = 0.8 / (6.0 * 0.0625)
VMEM = pltpu.VMEM


def call(body, outs, scratch=(), ins=None, limit=60 * 2**20):
    return pl.pallas_call(
        body,
        out_shape=outs,
        in_specs=ins,
        out_specs=jax.tree.map(lambda o: pl.BlockSpec(memory_space=VMEM), outs),
        scratch_shapes=list(scratch),
        compiler_params=pltpu.CompilerParams(vmem_limit_bytes=limit),
    )


def vm():
    return pl.BlockSpec(memory_space=VMEM)


def hbm():
    return pl.BlockSpec(memory_space=pl.ANY)


def shape(*dims):
    return jax.ShapeDtypeStruct(dims, f32)


def moved(value, axis, by):
    size = lax.axis_size(axis)
    return lax.ppermute(value, axis, [(i, (i + by) % size) for i in range(size)])


def lanes(rows):
    return lax.broadcasted_iota(jnp.int32, (rows, 128), 1)


def subs(rows):
    return lax.broadcasted_iota(jnp.int32, (rows, 128), 0)


def split_dot(x, w):
    high = x.astype(jnp.bfloat16)
    low = (x - high.astype(f32)).astype(jnp.bfloat16)
    return jnp.dot(high, w, preferred_element_type=f32) + jnp.dot(
        low, w, preferred_element_type=f32
    )


def star(tiles, above, below):
    count = len(tiles)
    rows = tiles[0].shape[0]
    lane = lanes(rows)
    ahead = [pltpu.roll(t, 127, 1) for t in tiles]
    behind = [pltpu.roll(t, 1, 1) for t in tiles]
    out = []
    for k in range(count):
        if count > 1:
            nxt = jnp.where(lane == 127, ahead[(k + 1) % count], ahead[k])
            prv = jnp.where(lane == 0, behind[(k - 1) % count], behind[k])
        else:
            nxt, prv = ahead[0], behind[0]
        t = tiles[k]
        total = (above[k] + below[k]) + (nxt + prv)
        total = total + (pltpu.roll(t, 1, 0) + pltpu.roll(t, rows - 1, 0))
        out.append(KEEP * t + SIDE * total)
    return out


def pack_y0(v, g, xh, xl, yf, yl, vf, vl, gf, gl, sems):
    copies = [
        pltpu.make_async_copy(v.at[:, 0:8], vf, sems.at[0]),
        pltpu.make_async_copy(v.at[:, 56:64], vl, sems.at[1]),
        pltpu.make_async_copy(g.at[:, 0:8], gf, sems.at[2]),
        pltpu.make_async_copy(g.at[:, 56:64], gl, sems.at[3]),
    ]
    for c in copies:
        c.start()
    sub = lax.broadcasted_iota(jnp.int32, (8, 256), 0)

    def put(p, a, b, c, d):
        yf[p] = jnp.where(sub < 4, a, pltpu.roll(b, 4, 0))
        yl[p] = jnp.where(sub < 4, pltpu.roll(d, 4, 0), c)

    for i in range(4):
        put(64 + i, xh[i, 0:8], xh[4 + i, 0:8], xh[i, 56:64], xh[4 + i, 56:64])
        put(68 + i, xl[i, 0:8], xl[4 + i, 0:8], xl[i, 56:64], xl[4 + i, 56:64])
    for c in copies:
        c.wait()

    @pl.loop(0, 64)
    def _(p):
        put(p, vf[p], gf[p], vl[p], gl[p])


def assemble0(v, g, xh, xl, yh, yl, a, gb, zf, zl, sums, sems):
    copies = []
    for k in range(2):
        lo = 128 * k
        copies.append(
            pltpu.make_async_copy(v.at[:, :, lo : lo + 128], a.at[0:64, k, 0:64], sems.at[k])
        )
        copies.append(
            pltpu.make_async_copy(g.at[:, :, lo : lo + 128], gb.at[0:64, k, 0:64], sems.at[2 + k])
        )
    for c in copies:
        c.start()
    sub = lax.broadcasted_iota(jnp.int32, (8, 128), 0)
    for k in range(2):
        cut = slice(128 * k, 128 * k + 128)
        for i in range(4):
            a[64 + i, k, 0:64] = xh[i, :, cut]
            a[68 + i, k, 0:64] = xl[i, :, cut]
            gb[64 + i, k, 0:64] = xh[4 + i, :, cut] * B0
            gb[68 + i, k, 0:64] = xl[4 + i, :, cut] * B0

    @pl.loop(0, 72)
    def _(p):
        for k in range(2):
            cut = slice(128 * k, 128 * k + 128)
            h = yh[p, :, cut]
            l = yl[p, :, cut]
            a[p, k, 64:72] = jnp.where(sub < 4, h, l)
            gb[p, k, 64:72] = pltpu.roll(jnp.where(sub < 4, l, h), 4, 0) * B0

    for c in copies:
        c.wait()

    def fold(x):
        return jnp.sum(x.reshape(8, 8, 128), axis=0)

    def scale(p, carry):
        sv, sg = carry
        for k in range(2):
            t = gb[p, k, 0:64] * B0
            gb[p, k, 0:64] = t
            sg = sg + fold(t)
            sv = sv + fold(a[p, k, 0:64])
        return sv, sg

    sv, sg = lax.fori_loop(0, 64, scale, (jnp.zeros((8, 128), f32), jnp.zeros((8, 128), f32)))
    sums[0] = sv
    sums[1] = sg
    lane = lanes(72)
    group = lane // 8
    is_g = (lane % 8) >= 4

    @pl.loop(0, 5)
    def _(q):
        first = jnp.zeros((72, 128), f32)
        last = jnp.zeros((72, 128), f32)
        for j in range(16):
            p = jnp.minimum(16 * q + j, 71)
            mv = (group == j) & ~is_g
            mg = (group == j) & is_g
            first = jnp.where(mv, pltpu.roll(a[p, 0], 8 * j, 1), first)
            first = jnp.where(mg, pltpu.roll(gb[p, 0], 8 * j + 4, 1), first)
            last = jnp.where(mv, pltpu.roll(a[p, 1], (8 * j + 4) % 128, 1), last)
            last = jnp.where(mg, pltpu.roll(gb[p, 1], (8 * j + 8) % 128, 1), last)
        zf[q] = first
        zl[q] = last


def down0(a, gb, zh, zl, rz, v2, v2h, gh, g1, ah, b, xr, xe, yr, w):
    lane = lanes(72)

    @pl.loop(0, 72)
    def _(p):
        q = p // 16
        j = p % 16
        h = zh[q]
        l = zl[q]
        ah[p] = jnp.where(
            lane < 64, pltpu.roll(h, (128 - 8 * j) % 128, 1), pltpu.roll(l, (252 - 8 * j) % 128, 1)
        )
        gh[p] = jnp.where(
            lane < 64, pltpu.roll(h, (252 - 8 * j) % 128, 1), pltpu.roll(l, (248 - 8 * j) % 128, 1)
        )

    def wrap(p):
        return jnp.where(p > 71, p - 72, p)

    @pl.loop(0, 72)
    def _(p):
        up = wrap(p + 1)
        dn = wrap(p + 71)
        t = star(
            [a[p, 0], a[p, 1], ah[p]], [a[up, 0], a[up, 1], ah[up]], [a[dn, 0], a[dn, 1], ah[dn]]
        )
        b[p, 0] = t[0] + gb[p, 0]
        b[p, 1] = t[1] + gb[p, 1]
        b[p, 2] = t[2] + gh[p]

    @pl.loop(0, 72)
    def _(p):
        up = wrap(p + 1)
        dn = wrap(p + 71)
        t = star(*[[b[i, k] for k in range(3)] for i in (p, up, dn)])
        v2[p, 0] = t[0] + gb[p, 0]
        v2[p, 1] = t[1] + gb[p, 1]
        v2h[p] = t[2] + gh[p]

    def rest(p):
        up = wrap(p + 1)
        dn = wrap(p + 71)
        here, above, below = [[v2[i, 0], v2[i, 1], v2h[i]] for i in (p, up, dn)]
        t = star(here, above, below)
        return [t[k] - here[k] + (gb[p, k] if k < 2 else gh[p]) for k in range(3)]

    first = rest(71)
    for k in range(3):
        b[0, k] = first[k]

    @pl.loop(0, 32)
    def _(i):
        mid = rest(2 * i)
        high = rest(2 * i + 1)
        for k in range(3):
            t = 0.25 / B0 * (b[0, k] + high[k]) + 0.5 / B0 * mid[k]
            b[0, k] = high[k]
            if k < 2:
                xr[pl.ds(pl.multiple_of(72 * i, 8), 72), 128 * k : 128 * k + 128] = t
            else:
                xe[pl.ds(pl.multiple_of(72 * i, 8), 72)] = t

    @pl.loop(0, 8)
    def _(c):
        at = pl.ds(pl.multiple_of(288 * c, 8), 288)
        edge = pltpu.roll(xe[at], 1, 1)
        yr[at] = split_dot(xr[at], rz[...]) + jnp.where(lanes(288) == 0, 0.25 * edge, 0.0)

    @pl.loop(0, 32)
    def _(i):
        base = pl.multiple_of(72 * i, 8)
        w[0:8] = yr[pl.ds(base + 64, 8)]
        w[8:72] = yr[pl.ds(base, 64)]
        g1[i] = 0.5 * w[pl.ds(8, 32, stride=2)] + 0.25 * (
            w[pl.ds(7, 32, stride=2)] + w[pl.ds(9, 32, stride=2)]
        )


def pack_y(own, high, low, yf, yl):
    n, h, l = own.shape[0], high.shape[0], low.shape[0]
    rows = own.shape[1]
    for ref, at in ((own, 0), (high, n), (low, n + h)):
        m = ref.shape[0]
        yf[at : at + m] = ref[:, 0:8]
        yl[at : at + m] = ref[:, rows - 8 : rows]


def pack_z(own, xh, xl, yh, yl, e, zf, zl, *, width):
    n, h, l = own.shape[0], xh.shape[0], xl.shape[0]
    rows = own.shape[1]
    planes = n + h + l
    e[0:n, 0:rows] = own[...]
    e[n : n + h, 0:rows] = xh[...]
    e[n + h : planes, 0:rows] = xl[...]
    e[:, rows : rows + 8] = yh[...]
    e[:, rows + 8 : rows + 16] = yl[...]
    group = lanes(rows + 16) // 8
    for q in range((planes + 15) // 16):
        first = jnp.zeros((rows + 16, 128), f32)
        last = first
        for j in range(min(16, planes - 16 * q)):
            t = e[16 * q + j]
            first = jnp.where(group == j, pltpu.roll(t, 8 * j, 1), first)
            last = jnp.where(group == j, pltpu.roll(t, (8 * j + 8 + 128 - width) % 128, 1), last)
        zf[q] = first
        zl[q] = last


def down1(e, zh, zl, rz, v2, g, g2, v1, xr, xe, yr, w):
    lane = lanes(48)
    for p in range(41):
        q, j = divmod(p, 16)
        h = pltpu.roll(zh[q], (128 - 8 * j) % 128, 1)
        l = pltpu.roll(zl[q], (120 - 8 * j) % 128, 1)
        edge = jnp.where(lane < 64, h, l) * B1
        main = e[p] * B1
        g[p, 0] = main
        g[p, 1] = edge

    def wrap(p):
        return jnp.where(p > 40, p - 41, p)

    def planes(ref, p):
        return [[ref[i, k] for k in range(2)] for i in (p, wrap(p + 1), wrap(p + 40))]

    @pl.loop(0, 41)
    def _(p):
        t = star(*planes(g, p))
        for k in range(2):
            v2[p, k] = t[k] + g[p, k]

    def rest(p):
        near = planes(v2, p)
        t = star(*near)
        return [t[k] - near[0][k] + g[p, k] for k in range(2)]

    first = rest(40)
    for k in range(2):
        v1[k] = first[k]

    @pl.loop(0, 16)
    def _(i):
        mid = rest(2 * i)
        high = rest(2 * i + 1)
        at = pl.ds(pl.multiple_of(48 * i, 8), 48)
        for k in range(2):
            t = 0.25 / B1 * (v1[k] + high[k]) + 0.5 / B1 * mid[k]
            v1[k] = high[k]
            if k == 0:
                xr[at] = t
            else:
                xe[at] = t

    edge = pltpu.roll(xe[...], 1, 1)
    yr[...] = split_dot(xr[...], rz[...]) + jnp.where(lanes(768) == 0, 0.25 * edge, 0.0)

    @pl.loop(0, 16)
    def _(i):
        base = pl.multiple_of(48 * i, 8)
        w[0:8] = yr[pl.ds(base + 40, 8)]
        w[8:40] = yr[pl.ds(base, 32)]
        g2[i] = 0.5 * w[pl.ds(8, 16, stride=2)] + 0.25 * (
            w[pl.ds(7, 16, stride=2)] + w[pl.ds(9, 16, stride=2)]
        )


def climb(
    e2, zh, zl, sums, p2, p1, v21, g1, v20, v20h, gb, gh, out,
    g2, s2, c2, q1, a1, b1, c1, q0, a0, b0, w1, w0,
):
    cells = 1.0 / 134217728.0
    mean_v = jnp.sum(jnp.sum(sums[0], axis=0, keepdims=True), axis=1, keepdims=True) * cells
    mean_g = jnp.sum(jnp.sum(sums[1], axis=0, keepdims=True), axis=1, keepdims=True) * (cells / B0)
    lane = lanes(32)
    for p in range(32):
        q, j = divmod(p, 16)
        h = pltpu.roll(zh[q], (64 - 8 * j) % 128, 1)
        l = pltpu.roll(zl[q], (120 - 8 * j) % 128, 1)
        t = jnp.where(lane < 64, e2[p], jnp.where(lane < 96, h, l))
        t = (t - mean_g) * B2
        g2[p] = t
        s2[p] = t

    def sweep2(src, dst):
        @pl.loop(0, 32)
        def _(p):
            up = (p + 1) % 32
            dn = (p + 31) % 32
            dst[p] = star([src[p]], [src[up]], [src[dn]])[0] + g2[p]

    sweep2(s2, c2)
    sweep2(c2, s2)
    sweep2(s2, c2)
    sweep2(c2, s2)
    sweep2(s2, c2)
    rows = c2[...].reshape(1024, 128) - 4.0 * B1 * mean_g
    wide = split_dot(rows, p2[...])
    for k in range(2):
        c1[0:1024, 128 * k : 128 * k + 128] = wide[:, 128 * k : 128 * k + 128]
    sub8 = subs(8)

    @pl.loop(0, 21)
    def _(i):
        p = jnp.where(i < 2, 30 + i, i - 2)
        base = pl.multiple_of(32 * p, 8)
        for k in range(2):
            cut = slice(128 * k, 128 * k + 128)
            tail = jnp.where(sub8 < 6, c1[pl.ds(base + 16, 8), cut], c1[pl.ds(base + 24, 8), cut])
            t = jnp.concatenate([c1[pl.ds(base, 16), cut], tail], axis=0)
            w1[pl.ds(0, 24, stride=2)] = t
            w1[pl.ds(1, 24, stride=2)] = 0.5 * (t + pltpu.roll(t, 23, 0))
            q1[i, k] = w1[...]

    @pl.loop(0, 20)
    def _(i):
        even = jnp.where(i < 2, 37 + 2 * i, 2 * i - 4)
        for k in range(2):
            lo = q1[i, k]
            hi = q1[i + 1, k]
            a1[even, k] = v21[even, k] + lo
            a1[even + 1, k] = v21[even + 1, k] + 0.5 * (lo + hi)

    for k in range(2):
        a1[36, k] = v21[36, k] + q1[20, k]

    def wrap1(p):
        return jnp.where(p > 40, p - 41, p)

    def sweep1(src, dst):
        @pl.loop(0, 41)
        def _(p):
            t = star(*[[src[i, k] for k in range(2)] for i in (p, wrap1(p + 1), wrap1(p + 40))])
            for k in range(2):
                dst[p, k] = t[k] + g1[p, k]

    sweep1(a1, b1)
    sweep1(b1, a1)
    drop = mean_v + 4.0 * B0 * mean_g

    @pl.loop(0, 35)
    def _(i):
        p = jnp.where(i == 0, 40, i - 1)
        x = jnp.concatenate([a1[p, 0], a1[p, 1]], axis=1) - drop
        wide = split_dot(x, p1[...])
        for k in range(3):
            t = wide[:, 128 * k : 128 * k + 128]
            tail = jnp.where(sub8 < 6, t[32:40], t[40:48])
            t = jnp.concatenate([t[0:32], tail], axis=0)
            w0[k, pl.ds(0, 40, stride=2)] = t
            w0[k, pl.ds(1, 40, stride=2)] = 0.5 * (t + pltpu.roll(t, 39, 0))
            q0[i, k, 0:64] = w0[k, 0:64]
            q0[i, k, 64:72] = jnp.where(sub8 < 4, w0[k, 64:72], w0[k, 72:80])

    @pl.loop(0, 34)
    def _(i):
        even = jnp.where(i == 0, 70, 2 * i - 2)
        for k in range(3):
            lo = q0[i, k]
            hi = q0[i + 1, k]
            base = v20[even, k] if k < 2 else v20h[even]
            base2 = v20[even + 1, k] if k < 2 else v20h[even + 1]
            a0[even, k] = base + lo
            a0[even + 1, k] = base2 + 0.5 * (lo + hi)

    def wrap0(p):
        return jnp.where(p > 71, p - 72, p)

    @pl.loop(0, 66)
    def _(i):
        p = jnp.where(i == 65, 71, i)
        t = star(*[[a0[x, k] for k in range(3)] for x in (p, wrap0(p + 1), wrap0(p + 71))])
        for k in range(3):
            b0[p, k] = t[k] + (gb[p, k] if k < 2 else gh[p])

    @pl.loop(0, 64)
    def _(p):
        t = star(*[[b0[x, k] for k in range(3)] for x in (p, wrap0(p + 1), wrap0(p + 71))])
        for k in range(2):
            out[p, :, 128 * k : 128 * k + 128] = (t[k] + gb[p, k])[0:64]


def ring_restrict(fine, coarse):
    w = np.zeros((fine, 128), np.float32)
    for i in range(coarse):
        for d, c in ((-1, 0.25), (0, 0.5), (1, 0.25)):
            z = 2 * i + d
            if z >= 0:
                w[z, i] = c
    return jnp.asarray(w, jnp.bfloat16)


def ring_prolong(coarse_width, coarse_ring, fine_width, fine_ring, low, high):
    w = np.zeros((coarse_ring, fine_ring), np.float32)
    for z in range(-low, fine_width + high):
        i, odd = divmod(z, 2)
        col = z % fine_ring
        if odd:
            w[i % coarse_ring, col] += 0.5
            w[(i + 1) % coarse_ring, col] += 0.5
        else:
            w[i % coarse_ring, col] += 1.0
    return jnp.asarray(w, jnp.bfloat16)


def shards(right_side, initial_guess):
    v, g = initial_guess, right_side
    xh = moved(jnp.concatenate([v[0:4], g[0:4]], 0), "gx", -1)
    xl = moved(jnp.concatenate([v[60:64], g[60:64]], 0), "gx", 1)
    yf, yl = call(
        pack_y0,
        [shape(72, 8, 256)] * 2,
        [VMEM((64, 8, 256), f32)] * 4 + [pltpu.SemaphoreType.DMA((4,))],
        [hbm(), hbm(), vm(), vm()],
    )(v, g, xh, xl)
    yh = moved(yf, "gy", -1)
    yl = moved(yl, "gy", 1)
    a, gb, zf, zl, sums = call(
        assemble0,
        [shape(72, 2, 72, 128)] * 2 + [shape(5, 72, 128)] * 2 + [shape(2, 8, 128)],
        [pltpu.SemaphoreType.DMA((4,))],
        [hbm(), hbm()] + [vm()] * 4,
    )(v, g, xh, xl, yh, yl)
    zh = moved(zf, "gz", -1)
    zl = moved(zl, "gz", 1)
    for axis, by in (("gx", 4), ("gx", 2), ("gx", 1), ("gy", 2), ("gy", 1), ("gz", 2), ("gz", 1)):
        sums = sums + moved(sums, axis, by)
    v20, v20h, gh, g1 = call(
        down0,
        [shape(72, 2, 72, 128), shape(72, 72, 128), shape(72, 72, 128), shape(32, 32, 128)],
        [
            VMEM((72, 72, 128), f32),
            VMEM((72, 3, 72, 128), f32),
            VMEM((2304, 256), f32),
            VMEM((2304, 128), f32),
            VMEM((2304, 128), f32),
            VMEM((80, 128), f32),
        ],
        [vm()] * 5,
    )(a, gb, zh, zl, ring_restrict(256, 128))
    xh = moved(g1[0:5], "gx", -1)
    xl = moved(g1[28:32], "gx", 1)
    yf, yl = call(pack_y, [shape(41, 8, 128)] * 2, (), [vm()] * 3)(g1, xh, xl)
    yh = moved(yf, "gy", -1)
    yl = moved(yl, "gy", 1)
    e1, zf, zl = call(
        lambda *r: pack_z(*r, width=128),
        [shape(41, 48, 128)] + [shape(3, 48, 128)] * 2,
        (),
        [vm()] * 5,
    )(g1, xh, xl, yh, yl)
    zh = moved(zf, "gz", -1)
    zl = moved(zl, "gz", 1)
    v21, g1b, g2 = call(
        down1,
        [shape(41, 2, 48, 128)] * 2 + [shape(16, 16, 128)],
        [
            VMEM((2, 48, 128), f32),
            VMEM((768, 128), f32),
            VMEM((768, 128), f32),
            VMEM((768, 128), f32),
            VMEM((48, 128), f32),
        ],
        [vm()] * 4,
    )(e1, zh, zl, ring_restrict(128, 64))
    xh = moved(g2[0:8], "gx", -1)
    xl = moved(g2[8:16], "gx", 1)
    yf, yl = call(pack_y, [shape(32, 8, 128)] * 2, (), [vm()] * 3)(g2, xh, xl)
    yh = moved(yf, "gy", -1)
    yl = moved(yl, "gy", 1)
    e2, zf, zl = call(
        lambda *r: pack_z(*r, width=64),
        [shape(32, 32, 128)] + [shape(2, 32, 128)] * 2,
        (),
        [vm()] * 5,
    )(g2, xh, xl, yh, yl)
    zh = moved(zf, "gz", -1)
    zl = moved(zl, "gz", 1)
    return call(
        climb,
        shape(64, 64, 256),
        [
            VMEM((32, 32, 128), f32),
            VMEM((32, 32, 128), f32),
            VMEM((32, 32, 128), f32),
            VMEM((21, 2, 48, 128), f32),
            VMEM((41, 2, 48, 128), f32),
            VMEM((41, 2, 48, 128), f32),
            VMEM((1024, 256), f32),
            VMEM((35, 3, 72, 128), f32),
            VMEM((72, 3, 72, 128), f32),
            VMEM((72, 3, 72, 128), f32),
            VMEM((48, 128), f32),
            VMEM((3, 80, 128), f32),
        ],
        [vm()] * 12,
    )(
        e2, zh, zl, sums,
        ring_prolong(64, 128, 128, 256, 4, 5),
        ring_prolong(128, 256, 256, 384, 4, 4),
        v21, g1b, v20, v20h, gb, gh,
    )


def solution(mesh):
    placed = P("gx", "gy", "gz")
    return jax.shard_map(
        shards, mesh=mesh, in_specs=(placed, placed), out_specs=placed, check_vma=False
    )
```

```python
import functools

import jax
import jax.numpy as jnp
from jax import lax
from jax.experimental import pallas as pl
from jax.experimental.pallas import tpu as pltpu
from jax.sharding import PartitionSpec as P
import numpy as np

f32 = jnp.float32
KEEP = 0.2
SIDE = 0.8 / 6.0
B0 = 0.8 / 6.0
B1 = 0.8 / (6.0 * 0.25)
B2 = 0.8 / (6.0 * 0.0625)
VMEM = pltpu.VMEM


def call(body, outs, scratch=(), ins=None, limit=8 * 2**20, where=VMEM, alias={}):
    return pl.pallas_call(
        body,
        out_shape=outs,
        in_specs=ins,
        out_specs=jax.tree.map(lambda o: pl.BlockSpec(memory_space=where), outs),
        scratch_shapes=list(scratch),
        input_output_aliases=alias,
        compiler_params=pltpu.CompilerParams(vmem_limit_bytes=limit),
    )


def vm():
    return pl.BlockSpec(memory_space=VMEM)


def hbm():
    return pl.BlockSpec(memory_space=pltpu.HBM)


def shape(*dims):
    return VMEM(dims, f32)


def plain(*dims):
    return jax.ShapeDtypeStruct(dims, f32)


def near(value):
    return pltpu.with_memory_space_constraint(value, VMEM)


def moved(value, axis, by):
    size = lax.axis_size(axis)
    return near(lax.ppermute(value, axis, [(i, (i + by) % size) for i in range(size)]))


def lanes(rows):
    return lax.broadcasted_iota(jnp.int32, (rows, 128), 1)


def subs(rows):
    return lax.broadcasted_iota(jnp.int32, (rows, 128), 0)


def split_dot(x, w):
    high = x.astype(jnp.bfloat16)
    low = (x - high.astype(f32)).astype(jnp.bfloat16)
    return jnp.dot(high, w, preferred_element_type=f32) + jnp.dot(
        low, w, preferred_element_type=f32
    )


def sweep(load, idx, tiles, count, emit):
    lane = lanes(8)
    for j in tiles:
        r = 8 + 8 * j
        col = [[load(p, k, r) for k in range(count)] for p in idx]
        got = []
        for u in range(len(idx) - 2):
            t = col[u + 1]
            ahead = [pltpu.roll(x, 127, 1) for x in t]
            behind = [pltpu.roll(x, 1, 1) for x in t]
            for k in range(count):
                if count > 1:
                    nxt = jnp.where(lane == 127, ahead[(k + 1) % count], ahead[k])
                    prv = jnp.where(lane == 0, behind[(k - 1) % count], behind[k])
                else:
                    nxt, prv = ahead[0], behind[0]
                total = (col[u][k] + col[u + 2][k]) + (nxt + prv)
                total = total + (load(idx[u + 1], k, r + 1) + load(idx[u + 1], k, r - 1))
                got.append((KEEP * t[k] + SIDE * total, t[k]))
        emit(j, got)


def ring(start, many, size):
    out = []
    for u in range(-1, many + 1):
        p = start + u
        p = jnp.where(p < 0, p + size, p)
        out.append(jnp.where(p >= size, p - size, p))
    return out


def put(store, p, k, j, last, value):
    store(p, k, 8 + 8 * j, value)
    if j == 0:
        store(p, k, 16 + 8 * last, value)
    if j == last:
        store(p, k, 0, value)


def reader(*refs):
    main = refs[0]

    def load(p, k, r):
        if len(refs) > 1 and k == main.shape[1]:
            return refs[1][p, pl.ds(r, 8)]
        return main[p, k, pl.ds(r, 8)]

    return load


def writer(*refs):
    main = refs[0]

    def store(p, k, r, value):
        if len(refs) > 1 and k == main.shape[1]:
            refs[1][p, pl.ds(r, 8)] = value
        else:
            main[p, k, pl.ds(r, 8)] = value

    return store


def rows_out(yf, yl, p, vf, gf, vl, gl):
    sub = lax.broadcasted_iota(jnp.int32, (8, 256), 0)
    yf[p] = jnp.where(sub < 4, vf, pltpu.roll(gf, 4, 0))
    yl[p] = jnp.where(sub < 4, pltpu.roll(gl, 4, 0), vl)


def pack_y0(v, g, yf, yl, vf, vl, gf, gl, sems):
    copies = [
        pltpu.make_async_copy(v.at[:, 0:8], vf, sems.at[0]),
        pltpu.make_async_copy(v.at[:, 56:64], vl, sems.at[1]),
        pltpu.make_async_copy(g.at[:, 0:8], gf, sems.at[2]),
        pltpu.make_async_copy(g.at[:, 56:64], gl, sems.at[3]),
    ]
    for c in copies:
        c.start()
    for c in copies:
        c.wait()

    @pl.loop(0, 64, unroll=4)
    def _(p):
        rows_out(yf, yl, p, vf[p], gf[p], vl[p], gl[p])


def pack_corner0(xh, xl, yf, yl):
    for n, x in ((0, xh), (4, xl)):
        for i in range(4):
            rows_out(
                yf, yl, n + i, x[i, 0:8], x[4 + i, 0:8], x[i, 56:64], x[4 + i, 56:64]
            )


def assemble0(v, g, xh, xl, a, gb, sums, sems):
    copies = []
    for n in range(4):
        at = slice(16 * n, 16 * n + 16)
        for k in range(2):
            cut = slice(128 * k, 128 * k + 128)
            copies.append(
                pltpu.make_async_copy(v.at[at, :, cut], a.at[at, k, 8:72], sems.at[n, k])
            )
            copies.append(
                pltpu.make_async_copy(g.at[at, :, cut], gb.at[at, k, 0:64], sems.at[n, 2 + k])
            )
    for c in copies:
        c.start()
    for k in range(2):
        cut = slice(128 * k, 128 * k + 128)
        for i in range(4):
            for p, x in ((64 + i, xh), (68 + i, xl)):
                a[p, k, 8:72] = x[i, :, cut]
                a[p, k, 80:88] = x[i, 0:8, cut]
                gb[p, k, 0:64] = x[4 + i, :, cut] * B0

    def fold(x):
        x = x[0:32] + x[32:64]
        x = x[0:16] + x[16:32]
        return x[0:8] + x[8:16]

    def scale(p, carry):
        sv, sg = carry
        for k in range(2):
            t = gb[p, k, 0:64] * B0
            gb[p, k, 0:64] = t
            sg = sg + fold(t)
            t = a[p, k, 8:72]
            a[p, k, 80:88] = t[0:8]
            sv = sv + fold(t)
        return sv, sg

    carry = (jnp.zeros((8, 128), f32), jnp.zeros((8, 128), f32))
    for n in range(4):
        for c in copies[4 * n : 4 * n + 4]:
            c.wait()
        carry = lax.fori_loop(16 * n, 16 * n + 16, scale, carry)
    sums[...] = jnp.concatenate(
        [jnp.sum(x, axis=0, keepdims=True) for x in carry] + [jnp.zeros((6, 128), f32)], axis=0
    )


def pack_z0(a_in, gb_in, yh, yl, ch, cl, a, gb, zf, zl):
    sub = lax.broadcasted_iota(jnp.int32, (8, 128), 0)

    def fill(p, h, l):
        for k in range(2):
            cut = slice(128 * k, 128 * k + 128)
            t = jnp.where(sub < 4, h[:, cut], l[:, cut])
            a[p, k, 72:80] = t
            a[p, k, 0:8] = t
            gb[p, k, 64:72] = pltpu.roll(jnp.where(sub < 4, l[:, cut], h[:, cut]), 4, 0) * B0

    @pl.loop(0, 64, unroll=4)
    def _(p):
        fill(p, yh[p], yl[p])

    for n in range(8):
        fill(64 + n, ch[n], cl[n])

    lane = lanes(72)
    group = lane // 8
    is_g = (lane % 8) >= 4

    @pl.loop(0, 5)
    def _(q):
        first = jnp.zeros((72, 128), f32)
        last = jnp.zeros((72, 128), f32)
        for j in range(16):
            p = jnp.minimum(16 * q + j, 71)
            mine = group == j
            u = jnp.where(is_g, pltpu.roll(gb[p, 0], (8 * j + 4) % 128, 1), pltpu.roll(a[p, 0, 8:80], 8 * j, 1))
            w = jnp.where(
                is_g,
                pltpu.roll(gb[p, 1], (8 * j + 8) % 128, 1),
                pltpu.roll(a[p, 1, 8:80], (8 * j + 4) % 128, 1),
            )
            first = jnp.where(mine, u, first)
            last = jnp.where(mine, w, last)
        zf[q] = first
        zl[q] = last


def spread(own, nxt, prv):
    return jnp.concatenate([own + nxt + prv, nxt], axis=0)


def closed(own, nxt):
    parts = []
    for r in range(0, own.shape[0], 4):
        parts.append(own[r : r + 2] + nxt[r + 2 : r + 4])
    return parts[0] if len(parts) == 1 else jnp.concatenate(parts, axis=0)


def down0(a, gb, zh, zl, rz, s0, s4, v2, v2h, gh, g1, xf, xl, own, ah, b, last, xr, xe, yr, w):
    q0 = s0[0:2] + s4[0:2]
    own[0:2] = q0
    xf[5, 0:2] = q0
    xl[4, 0:2] = q0

    lane = lanes(72)

    @pl.loop(0, 72, unroll=4)
    def _(p):
        q = p // 16
        j = p % 16
        h = zh[q]
        l = zl[q]
        t = jnp.where(
            lane < 64, pltpu.roll(h, (128 - 8 * j) % 128, 1), pltpu.roll(l, (252 - 8 * j) % 128, 1)
        )
        ah[p, 8:80] = t
        ah[p, 0:8] = t[64:72]
        ah[p, 80:88] = t[0:8]
        gh[p] = jnp.where(
            lane < 64, pltpu.roll(h, (252 - 8 * j) % 128, 1), pltpu.roll(l, (248 - 8 * j) % 128, 1)
        )

    gload = reader(gb, gh)

    def relax(load, store):
        @pl.loop(0, 18)
        def _(i):
            idx = ring(4 * i, 4, 72)

            def emit(j, got):
                for n, (value, _) in enumerate(got):
                    u, k = divmod(n, 3)
                    put(store, idx[u + 1], k, j, 8, value + gload(idx[u + 1], k, 8 * j))

            sweep(load, idx, range(9), 3, emit)

    relax(reader(a, ah), writer(b))
    relax(reader(b), writer(v2, v2h))
    load = reader(v2, v2h)

    def rest(n, got, idx, j):
        u, k = divmod(n, 3)
        value, here = got[n]
        return value - here + gload(idx[u + 1], k, 8 * j)

    edge = ring(71, 1, 72)

    def emit_edge(j, got):
        for k in range(3):
            last[k, pl.ds(8 * j, 8)] = rest(k, got, edge, j)

    sweep(load, edge, range(9), 3, emit_edge)

    @pl.loop(0, 16)
    def _(i):
        idx = ring(4 * i, 4, 72)

        def emit(j, got):
            for k in range(3):
                r = [rest(3 * u + k, got, idx, j) for u in range(4)]
                rows = pl.ds(8 * j, 8)
                even = 0.25 / B0 * (last[k, rows] + r[1]) + 0.5 / B0 * r[0]
                odd = 0.25 / B0 * (r[1] + r[3]) + 0.5 / B0 * r[2]
                last[k, rows] = r[3]
                for n, t in ((0, even), (1, odd)):
                    at = pl.ds(pl.multiple_of(72 * (2 * i + n) + 8 * j, 8), 8)
                    if k < 2:
                        xr[at, 128 * k : 128 * k + 128] = t
                    else:
                        xe[at] = t

        sweep(load, idx, range(9), 3, emit)

    @pl.loop(0, 8)
    def _(c):
        at = pl.ds(pl.multiple_of(288 * c, 8), 288)
        edge = pltpu.roll(xe[at], 1, 1)
        yr[at] = split_dot(xr[at], rz[...]) + jnp.where(lanes(288) == 0, 0.25 * edge, 0.0)

    @pl.loop(0, 32)
    def _(i):
        base = pl.multiple_of(72 * i, 8)
        w[0:8] = yr[pl.ds(base + 64, 8)]
        w[8:72] = yr[pl.ds(base, 64)]
        g1[i] = 0.5 * w[pl.ds(8, 32, stride=2)] + 0.25 * (
            w[pl.ds(7, 32, stride=2)] + w[pl.ds(9, 32, stride=2)]
        )

    xf[0:5] = g1[0:5]
    xl[0:4] = g1[28:32]


def pack_y(own, xh, xl, q, yf, yl, qo, *, high, low, first_round):
    n, rows = own.shape[0], own.shape[1]
    for ref, at, m in ((own, 0, n), (xh, n, high), (xl, n + high, low)):
        yf[at : at + m] = ref[0:m, 0:8]
        yl[at : at + m] = ref[0:m, rows - 8 : rows]
    if first_round:
        t = spread(q[0:2], xh[high, 0:2], xl[low, 0:2])
    else:
        t = closed(q[0:16], xh[high, 0:16])
    m = t.shape[0]
    yf[n + high + low, 0:m] = t
    yl[n + high + low, 0:m] = t
    qo[0:m] = t


def pack_z(own, xh, xl, yh, yl, q, e, zf, zl, qo, *, width, high, low, first_round):
    n, rows = own.shape[0], own.shape[1]
    planes = n + high + low
    e[0:n, 0:rows] = own[...]
    e[n : n + high, 0:rows] = xh[0:high]
    e[n + high : planes, 0:rows] = xl[0:low]
    e[:, rows : rows + 8] = yh[0:planes]
    e[:, rows + 8 : rows + 16] = yl[0:planes]
    group = lanes(rows + 16) // 8
    groups = (planes + 15) // 16
    for i in range(groups):
        first = jnp.zeros((rows + 16, 128), f32)
        last = first
        for j in range(min(16, planes - 16 * i)):
            t = e[16 * i + j]
            first = jnp.where(group == j, pltpu.roll(t, 8 * j, 1), first)
            last = jnp.where(group == j, pltpu.roll(t, (8 * j + 8 + 128 - width) % 128, 1), last)
        zf[i] = first
        zl[i] = last
    if first_round:
        t = spread(q[0:4], yh[planes, 0:4], yl[planes, 0:4])
    else:
        t = closed(q[0:8], yh[planes, 0:8])
    m = t.shape[0]
    zf[groups, 0:m] = t
    zl[groups, 0:m] = t
    qo[0:m] = t


def down1(e, zh, zl, rz, q, v2, g, g2, xf, xl, own, last, xr, xe, yr, w):
    t = spread(q[0:8], zh[3, 0:8], zl[3, 0:8])
    own[...] = t
    xf[8] = t
    lane = lanes(48)
    gput = writer(g)
    for p in range(41):
        c, i = divmod(p, 16)
        h = pltpu.roll(zh[c], (128 - 8 * i) % 128, 1)
        l = pltpu.roll(zl[c], (120 - 8 * i) % 128, 1)
        tile = [e[p] * B1, jnp.where(lane < 64, h, l) * B1]
        for k in range(2):
            for j in range(6):
                put(gput, p, k, j, 5, tile[k][8 * j : 8 * j + 8])
    gload = reader(g)
    store = writer(v2)

    def relax(first, many):
        idx = ring(first, many, 41)

        def emit(j, got):
            for n, (value, _) in enumerate(got):
                u, k = divmod(n, 2)
                put(store, idx[u + 1], k, j, 5, value + gload(idx[u + 1], k, 8 + 8 * j))

        sweep(gload, idx, range(6), 2, emit)

    pl.loop(0, 10)(lambda i: relax(4 * i, 4))
    relax(40, 1)
    load = reader(v2)

    def rest(n, got, idx, j):
        u, k = divmod(n, 2)
        value, here = got[n]
        return value - here + gload(idx[u + 1], k, 8 + 8 * j)

    edge = ring(40, 1, 41)

    def emit_edge(j, got):
        for k in range(2):
            last[k, pl.ds(8 * j, 8)] = rest(k, got, edge, j)

    sweep(load, edge, range(6), 2, emit_edge)

    @pl.loop(0, 8)
    def _(i):
        idx = ring(4 * i, 4, 41)

        def emit(j, got):
            for k in range(2):
                r = [rest(2 * u + k, got, idx, j) for u in range(4)]
                rows = pl.ds(8 * j, 8)
                even = 0.25 / B1 * (last[k, rows] + r[1]) + 0.5 / B1 * r[0]
                odd = 0.25 / B1 * (r[1] + r[3]) + 0.5 / B1 * r[2]
                last[k, rows] = r[3]
                for n, t in ((0, even), (1, odd)):
                    at = pl.ds(pl.multiple_of(48 * (2 * i + n) + 8 * j, 8), 8)
                    if k == 0:
                        xr[at] = t
                    else:
                        xe[at] = t

        sweep(load, idx, range(6), 2, emit)

    edge = pltpu.roll(xe[...], 1, 1)
    yr[...] = split_dot(xr[...], rz[...]) + jnp.where(lanes(768) == 0, 0.25 * edge, 0.0)

    @pl.loop(0, 16)
    def _(i):
        base = pl.multiple_of(48 * i, 8)
        w[0:8] = yr[pl.ds(base + 40, 8)]
        w[8:40] = yr[pl.ds(base, 32)]
        g2[i] = 0.5 * w[pl.ds(8, 16, stride=2)] + 0.25 * (
            w[pl.ds(7, 16, stride=2)] + w[pl.ds(9, 16, stride=2)]
        )

    xf[0:8] = g2[0:8]
    xl[...] = g2[8:16]


def climb(
    e2, zh, zl, sums, p2, p1, v21, g1, v20, v20h, gb, gh, out,
    g2, s2, c2, c1, q1, a1, b1, x1, y1, a0, b0, w1, w0, sems,
):
    cells = 1.0 / 134217728.0
    total = jnp.sum(closed(sums[0:4], zh[2, 0:4]), axis=1, keepdims=True)
    mean_v = total[0:1] * cells
    mean_g = total[1:2] * (cells / B0)
    lane = lanes(32)
    sput = writer(s2)
    for p in range(32):
        q, i = divmod(p, 16)
        h = pltpu.roll(zh[q], (64 - 8 * i) % 128, 1)
        l = pltpu.roll(zl[q], (120 - 8 * i) % 128, 1)
        t = jnp.where(lane < 64, e2[p], jnp.where(lane < 96, h, l))
        t = (t - mean_g) * B2
        g2[p] = t
        for j in range(4):
            put(sput, p, 0, j, 3, t[8 * j : 8 * j + 8])

    def sweep2(src, dst):
        load, store = reader(src), writer(dst)

        @pl.loop(0, 4)
        def _(i):
            idx = [(8 * i + u + 31) % 32 for u in range(10)]

            def emit(j, got):
                for u, (value, _) in enumerate(got):
                    put(store, idx[u + 1], 0, j, 3, value + g2[idx[u + 1], pl.ds(8 * j, 8)])

            sweep(load, idx, range(4), 1, emit)

    sweep2(s2, c2)
    sweep2(c2, s2)
    sweep2(s2, c2)
    sweep2(c2, s2)
    sweep2(s2, c2)
    rows = c2[:, 0, 8:40].reshape(1024, 128) - 4.0 * B1 * mean_g
    c1[...] = split_dot(rows, p2[...])
    sub8 = subs(8)

    for i in range(21):
        base = 32 * ((i + 30) % 32)
        for k in range(2):
            cut = slice(128 * k, 128 * k + 128)
            tail = jnp.where(sub8 < 6, c1[base + 16 : base + 24, cut], c1[base + 24 : base + 32, cut])
            t = jnp.concatenate([c1[base : base + 16, cut], tail], axis=0)
            w1[i % 2, k, pl.ds(0, 24, stride=2)] = t
            w1[i % 2, k, pl.ds(1, 24, stride=2)] = 0.5 * (t + pltpu.roll(t, 23, 0))
            q1[i, k] = w1[i % 2, k]

    aput = writer(a1)

    @pl.loop(0, 20, unroll=4)
    def _(i):
        even = jnp.where(i < 2, 37 + 2 * i, 2 * i - 4)
        for k in range(2):
            for j in range(6):
                at = pl.ds(8 * j, 8)
                here = pl.ds(8 * j + 8, 8)
                lo = q1[i, k, at]
                hi = q1[i + 1, k, at]
                put(aput, even, k, j, 5, v21[even, k, here] + lo)
                put(aput, even + 1, k, j, 5, v21[even + 1, k, here] + 0.5 * (lo + hi))

    for k in range(2):
        for j in range(6):
            put(aput, 36, k, j, 5, v21[36, k, 8 * j + 8 : 8 * j + 16] + q1[20, k, 8 * j : 8 * j + 8])

    def sweep1(src, dst):
        load, store = reader(src), writer(dst)

        def relax(first, many):
            idx = ring(first, many, 41)

            def emit(j, got):
                for n, (value, _) in enumerate(got):
                    u, k = divmod(n, 2)
                    put(
                        store, idx[u + 1], k, j, 5,
                        value + g1[idx[u + 1], k, pl.ds(8 * j + 8, 8)],
                    )

            sweep(load, idx, range(6), 2, emit)

        pl.loop(0, 10)(lambda i: relax(4 * i, 4))
        relax(40, 1)

    sweep1(a1, b1)
    sweep1(b1, a1)
    drop = mean_v + 4.0 * B0 * mean_g

    @pl.loop(0, 5)
    def _(c):
        for n in range(7):
            i = 7 * c + n
            p = jnp.where(i == 0, 40, i - 1)
            for k in range(2):
                x1[48 * n : 48 * n + 48, 128 * k : 128 * k + 128] = a1[p, k, 8:56] - drop
        y1[...] = split_dot(x1[...], p1[...])
        for n in range(7):
            i = 7 * c + n
            for k in range(3):
                cut = slice(128 * k, 128 * k + 128)
                tail = jnp.where(
                    sub8 < 6,
                    y1[48 * n + 32 : 48 * n + 40, cut],
                    y1[48 * n + 40 : 48 * n + 48, cut],
                )
                t = jnp.concatenate([y1[48 * n : 48 * n + 32, cut], tail], axis=0)
                w0[n % 2, k, pl.ds(0, 40, stride=2)] = t
                w0[n % 2, k, pl.ds(1, 40, stride=2)] = 0.5 * (t + pltpu.roll(t, 39, 0))
                b0[i, k, 0:64] = w0[n % 2, k, 0:64]
                b0[i, k, 64:72] = jnp.where(sub8 < 4, w0[n % 2, k, 64:72], w0[n % 2, k, 72:80])

    fload = reader(v20, v20h)
    fput = writer(a0)

    @pl.loop(0, 34, unroll=2)
    def _(i):
        even = jnp.where(i == 0, 70, 2 * i - 2)
        for k in range(3):
            for j in range(9):
                lo = b0[i, k, 8 * j : 8 * j + 8]
                hi = b0[i + 1, k, 8 * j : 8 * j + 8]
                put(fput, even, k, j, 8, fload(even, k, 8 * j + 8) + lo)
                put(fput, even + 1, k, j, 8, fload(even + 1, k, 8 * j + 8) + 0.5 * (lo + hi))

    gload = reader(gb, gh)
    aload, bput, bload = reader(a0), writer(b0), reader(b0)

    @pl.loop(0, 17)
    def _(i):
        idx = ring(4 * i - 1, 4, 72)

        def emit(j, got):
            for n, (value, _) in enumerate(got):
                u, k = divmod(n, 3)
                put(bput, idx[u + 1], k, j, 8, value + gload(idx[u + 1], k, 8 * j))

        sweep(aload, idx, range(9), 3, emit)

    def push(i, k):
        at = pl.ds(4 * i, 4)
        cut = pl.ds(128 * k, 128)
        return pltpu.make_async_copy(a0.at[at, k, 8:72], out.at[at, :, cut], sems.at[i, k])

    @pl.loop(0, 16)
    def _(i):
        idx = ring(4 * i, 4, 72)

        def emit(j, got):
            for n, (value, _) in enumerate(got):
                u, k = divmod(n, 3)
                if k < 2:
                    p = 4 * i + u
                    a0[p, k, pl.ds(8 * j + 8, 8)] = value + gb[p, k, pl.ds(8 * j, 8)]

        sweep(bload, idx, range(8), 3, emit)
        for k in range(2):
            push(i, k).start()

    @pl.loop(0, 16)
    def _(i):
        for k in range(2):
            push(i, k).wait()


def ring_restrict(fine, coarse):
    w = np.zeros((fine, 128), np.float32)
    for i in range(coarse):
        for d, c in ((-1, 0.25), (0, 0.5), (1, 0.25)):
            z = 2 * i + d
            if z >= 0:
                w[z, i] = c
    return jnp.asarray(w, jnp.bfloat16)


def ring_prolong(coarse_width, coarse_ring, fine_width, fine_ring, low, high):
    w = np.zeros((coarse_ring, fine_ring), np.float32)
    for z in range(-low, fine_width + high):
        i, odd = divmod(z, 2)
        col = z % fine_ring
        if odd:
            w[i % coarse_ring, col] += 0.5
            w[(i + 1) % coarse_ring, col] += 0.5
        else:
            w[i % coarse_ring, col] += 1.0
    return jnp.asarray(w, jnp.bfloat16)


def shards(right_side, initial_guess):
    v, g = initial_guess, right_side
    bf = functools.partial
    xh = moved(jnp.concatenate([v[0:4], g[0:4]], 0), "gx", -1)
    xl = moved(jnp.concatenate([v[60:64], g[60:64]], 0), "gx", 1)
    yf, yl = call(
        pack_y0,
        [shape(64, 8, 256)] * 2,
        [VMEM((64, 8, 256), f32)] * 4 + [pltpu.SemaphoreType.DMA((4,))],
        [hbm(), hbm()],
    )(v, g)
    yh = moved(yf, "gy", -1)
    yl = moved(yl, "gy", 1)
    cf, cl = call(pack_corner0, [shape(8, 8, 256)] * 2, (), [vm()] * 2)(xh, xl)
    ch = moved(cf, "gy", -1)
    cl = moved(cl, "gy", 1)
    a, gb, sums = call(
        assemble0,
        [shape(72, 2, 88, 128), shape(72, 2, 72, 128), shape(8, 128)],
        [pltpu.SemaphoreType.DMA((4, 4))],
        [hbm(), hbm()] + [vm()] * 2,
    )(v, g, xh, xl)
    far = moved(sums, "gx", 4)
    a, gb, zf, zl = call(
        pack_z0,
        [shape(72, 2, 88, 128), shape(72, 2, 72, 128)] + [shape(5, 72, 128)] * 2,
        (),
        [vm()] * 6,
        alias={0: 0, 1: 1},
    )(a, gb, yh, yl, ch, cl)
    zh = moved(zf, "gz", -1)
    zl = moved(zl, "gz", 1)
    v20, v20h, gh, g1, xf, xl, own = call(
        down0,
        [
            shape(72, 2, 88, 128),
            shape(72, 88, 128),
            shape(72, 72, 128),
            shape(32, 32, 128),
            shape(6, 32, 128),
            shape(5, 32, 128),
            shape(8, 128),
        ],
        [
            VMEM((72, 88, 128), f32),
            VMEM((72, 3, 88, 128), f32),
            VMEM((3, 72, 128), f32),
            VMEM((2304, 256), f32),
            VMEM((2304, 128), f32),
            VMEM((2304, 128), f32),
            VMEM((80, 128), f32),
        ],
        [vm()] * 7,
        limit=24 * 2**20,
        alias={0: 0},
    )(a, gb, zh, zl, ring_restrict(256, 128), sums, far)
    xh = moved(xf, "gx", -1)
    xl = moved(xl, "gx", 1)
    yf, yl, own = call(
        bf(pack_y, high=5, low=4, first_round=True),
        [shape(42, 8, 128)] * 2 + [shape(8, 128)],
        (),
        [vm()] * 4,
    )(g1, xh, xl, own)
    yh = moved(yf, "gy", -1)
    yl = moved(yl, "gy", 1)
    e1, zf, zl, own = call(
        bf(pack_z, width=128, high=5, low=4, first_round=True),
        [shape(41, 48, 128)] + [shape(4, 48, 128)] * 2 + [shape(8, 128)],
        (),
        [vm()] * 6,
    )(g1, xh, xl, yh, yl, own)
    zh = moved(zf, "gz", -1)
    zl = moved(zl, "gz", 1)
    v21, g1b, g2, xf, xl, own = call(
        down1,
        [shape(41, 2, 64, 128)] * 2
        + [shape(16, 16, 128), shape(9, 16, 128), shape(8, 16, 128), shape(16, 128)],
        [
            VMEM((2, 48, 128), f32),
            VMEM((768, 128), f32),
            VMEM((768, 128), f32),
            VMEM((768, 128), f32),
            VMEM((48, 128), f32),
        ],
        [vm()] * 5,
    )(e1, zh, zl, ring_restrict(128, 64), own)
    xh = moved(xf, "gx", -1)
    xl = moved(xl, "gx", 1)
    yf, yl, own = call(
        bf(pack_y, high=8, low=8, first_round=False),
        [shape(33, 8, 128)] * 2 + [shape(8, 128)],
        (),
        [vm()] * 4,
    )(g2, xh, xl, own)
    yh = moved(yf, "gy", -1)
    yl = moved(yl, "gy", 1)
    e2, zf, zl, sums = call(
        bf(pack_z, width=64, high=8, low=8, first_round=False),
        [shape(32, 32, 128)] + [shape(3, 32, 128)] * 2 + [shape(8, 128)],
        (),
        [vm()] * 6,
    )(g2, xh, xl, yh, yl, own)
    zh = moved(zf, "gz", -1)
    zl = moved(zl, "gz", 1)
    return call(
        climb,
        jax.ShapeDtypeStruct((64, 64, 256), f32),
        [
            VMEM((32, 32, 128), f32),
            VMEM((32, 1, 48, 128), f32),
            VMEM((32, 1, 48, 128), f32),
            VMEM((1024, 256), f32),
            VMEM((21, 2, 48, 128), f32),
            VMEM((41, 2, 64, 128), f32),
            VMEM((41, 2, 64, 128), f32),
            VMEM((336, 256), f32),
            VMEM((336, 384), f32),
            VMEM((72, 3, 88, 128), f32),
            VMEM((72, 3, 88, 128), f32),
            VMEM((2, 2, 48, 128), f32),
            VMEM((2, 3, 80, 128), f32),
            pltpu.SemaphoreType.DMA((16, 2)),
        ],
        [vm()] * 12,
        limit=40 * 2**20,
        where=pltpu.HBM,
    )(
        e2, zh, zl, sums,
        ring_prolong(64, 128, 128, 256, 4, 5),
        ring_prolong(128, 256, 256, 384, 4, 4),
        v21, g1b, v20, v20h, gb, gh,
    )


def solution(mesh):
    placed = P("gx", "gy", "gz")
    return jax.shard_map(
        shards, mesh=mesh, in_specs=(placed, placed), out_specs=placed, check_vma=False
    )
```
